32 devices in a mesh: depth: 8 (over y, x, core), plane: 4 (over z).
Axes of the slice: x: 2, y: 2, z: 4, core: 2. Of those that a mesh axis runs over, the one named last changes fastest.
Arguments:
- activations: bfloat16 [8, 8, 64, 1024], P('plane', 'depth'), may hold values from -6 to 6
- plane_weight: bfloat16 [2, 3, 64, 576], replicated, may hold values from -0.375 to 0.375
- plane_bias: float32 [2, 3, 64], replicated, may hold values from -3 to 3
- depth_weight: bfloat16 [2, 64, 192], replicated, may hold values from -0.75 to 0.75
- depth_bias: float32 [2, 64], replicated, may hold values from -3 to 3
- counts: int32 [4], replicated, may hold values from 1 to 2, as said below
- neighbours: int32 [8, 8], P('plane'), may hold values from -1 to 7, as said below
- voxel_mask: int32 [8, 8, 1024], P('plane', 'depth'), may hold values from 0 to 1, as said below
Outputs:
- hidden: bfloat16 [8, 8, 64, 1024], P('plane', 'depth')
The draws below stay inside these ranges and needn't reach their ends.
Inputs may be any that keep to these rules, and one draw needn't show every extreme that they name: `counts`: each entry is between 1 and 2; at least one entry equals 2. `neighbours`: for a live slot, the live slot that holds the adjacent tile of a grid in that direction, or -1; all -1 for dead slots; neighbourhood is symmetric. `voxel_mask`: zero in dead slots.
All inputs are finite; a program needn't handle non-finite values.
Results may differ from the reference program's by a relative error of at most 0.008.
Values may be sent and summed in bfloat16 or wider, within the bound.
No kernel may reach another device: no remote copies, remote signals or barrier semaphores. Data moves between devices by JAX's collectives and lax.ppermute only.
A program may use at most 64 MiB of HBM per device.

```python
import jax
import jax.numpy as jnp
from jax import lax

CHANNELS = 64
TILE = 32
BLOCKS = 2
SLOTS = 2
CELLS = 1024
DEPTH = 8
N_PLANE = 4


def layout(key):
    base_key = jax.random.fold_in(key, 7)
    count_key, owner_key, place_key = jax.random.split(base_key, 3)
    counts = jax.random.randint(count_key, (N_PLANE,), 1, SLOTS + 1)
    full_owner = jax.random.randint(owner_key, (), 0, N_PLANE)
    counts = jnp.where(jnp.arange(N_PLANE) == full_owner, SLOTS, counts).astype(jnp.int32)
    tile_total = N_PLANE * SLOTS
    cell_of = jax.random.permutation(place_key, tile_total)
    cell_tile = jnp.argsort(cell_of, stable=True)
    tile_ids = jnp.arange(tile_total)
    alive = tile_ids % SLOTS < counts[tile_ids // SLOTS]
    grid_row = cell_of // SLOTS
    grid_col = cell_of % SLOTS
    columns = []
    for row_step, col_step in [(-1, -1), (-1, 0), (-1, 1), (0, -1), (0, 1), (1, -1), (1, 0), (1, 1)]:
        new_row = grid_row + row_step
        new_col = grid_col + col_step
        inside = (new_row >= 0) & (new_row < N_PLANE) & (new_col >= 0) & (new_col < SLOTS)
        cell_index = jnp.clip(new_row, 0, N_PLANE - 1) * SLOTS + jnp.clip(new_col, 0, SLOTS - 1)
        other_tile = cell_tile[cell_index]
        linked = inside & alive & alive[other_tile]
        columns.append(jnp.where(linked, other_tile, -1))
    return (counts, jnp.stack(columns, -1).astype(jnp.int32), alive)


def draw_activations(key, part):
    base_key = jax.random.fold_in(key, 23)
    offset_key, noise_key = jax.random.split(base_key, 2)
    tile_total = N_PLANE * SLOTS
    full_shape = (tile_total, DEPTH, CHANNELS, CELLS)
    offsets = jax.random.uniform(offset_key, (tile_total, 1, CHANNELS, 1), jnp.float32, -2.5, 2.5)
    noise = jax.random.normal(noise_key, full_shape, jnp.float32)
    return jnp.clip(offsets + noise, -6.0, 6.0).astype(jnp.bfloat16)


def draw_counts(key, part):
    return layout(key)[0]


def draw_neighbours(key, part):
    return layout(key)[1]


def draw_voxel_mask(key, part):
    alive = layout(key)[2]
    random_bits = jax.random.randint(jax.random.fold_in(key, 11), (N_PLANE * SLOTS, DEPTH, CELLS), 0, 5)
    inside = (random_bits > 0) & alive[:, None, None]
    return jnp.where(inside, 1, 0).astype(jnp.int32)


def normal_values(rng, extent, width, reach, kind=jnp.bfloat16):
    drawn = width * jax.random.normal(rng, extent, jnp.float32)
    return jnp.clip(drawn, min=-reach, max=reach).astype(kind)


def setup_inputs(seed: int = 0) -> dict:
    splits = jax.random.split(jax.random.key(seed), 9)
    return {
        "activations": draw_activations(jax.random.fold_in(splits[8], 71), 0),
        "plane_weight": normal_values(splits[1], (BLOCKS, 3, CHANNELS, 9 * CHANNELS), (4 * CHANNELS) ** -0.5, 0.375),
        "plane_bias": normal_values(splits[2], (BLOCKS, 3, CHANNELS), 0.5, 3.0, jnp.float32),
        "depth_weight": normal_values(splits[3], (BLOCKS, CHANNELS, 3 * CHANNELS), CHANNELS ** -0.5, 0.75),
        "depth_bias": normal_values(splits[4], (BLOCKS, CHANNELS), 0.5, 3.0, jnp.float32),
        "counts": draw_counts(jax.random.fold_in(splits[8], 71), 0),
        "neighbours": draw_neighbours(jax.random.fold_in(splits[8], 71), 0),
        "voxel_mask": draw_voxel_mask(jax.random.fold_in(splits[8], 71), 0),
    }


def flatten(array):
    return array.reshape(array.shape[:-2] + (-1,))


def strips(tile_view, strip_width):
    top_rows = tile_view[..., :strip_width, :]
    bottom = tile_view[..., TILE - strip_width:, :]
    left_cols = tile_view[..., :, :strip_width]
    right_cols = tile_view[..., :, TILE - strip_width:]
    return jnp.concatenate([flatten(top_rows), flatten(bottom), flatten(left_cols), flatten(right_cols)], -1)


def surround(center, neighbour_table, strip_pool, strip_width):
    length = strip_width * TILE
    present = neighbour_table >= 0
    safe_index = jnp.maximum(neighbour_table, 0)

    def fetch_strip(column, segment, piece_shape):
        pieces = strip_pool[safe_index[:, column]][..., segment * length:(segment + 1) * length]
        pieces = pieces.reshape(pieces.shape[:-1] + piece_shape)
        keep = present[:, column].reshape((-1,) + (1,) * (pieces.ndim - 1))
        return jnp.where(keep, pieces, jnp.zeros_like(pieces))

    rows_shape = (strip_width, TILE)
    cols_shape = (TILE, strip_width)
    north_west = fetch_strip(0, 1, rows_shape)[..., TILE - strip_width:]
    north = fetch_strip(1, 1, rows_shape)
    north_east = fetch_strip(2, 1, rows_shape)[..., :strip_width]
    west_side = fetch_strip(3, 3, cols_shape)
    east_side = fetch_strip(4, 2, cols_shape)
    south_west = fetch_strip(5, 0, rows_shape)[..., TILE - strip_width:]
    south_side = fetch_strip(6, 0, rows_shape)
    south_east = fetch_strip(7, 0, rows_shape)[..., :strip_width]
    upper_band = jnp.concatenate([north_west, north, north_east], -1)
    middle = jnp.concatenate([west_side, center, east_side], -1)
    lower_band = jnp.concatenate([south_west, south_side, south_east], -1)
    return jnp.concatenate([upper_band, middle, lower_band], -2)


def plane_conv(padded, weight):
    inner = padded.shape[-1] - 2
    tap_list = [padded[..., row_off:row_off + inner, col_off:col_off + inner] for row_off in range(3) for col_off in range(3)]
    stacked = jnp.concatenate(tap_list, axis=-3)
    stacked = stacked.reshape(stacked.shape[:-2] + (inner * inner,))
    return jnp.einsum("ok,nskq->nsoq", weight.astype(jnp.float32), stacked.astype(jnp.float32))


def reference(activations, plane_weight, plane_bias, depth_weight, depth_bias, counts, neighbours, voxel_mask):
    tile_ids = jnp.arange(N_PLANE * SLOTS, dtype=jnp.int32)
    alive = (tile_ids % SLOTS) < counts[tile_ids // SLOTS]
    hidden = jnp.where(alive[:, None, None, None], activations, jnp.zeros_like(activations))
    mask_f = voxel_mask.astype(jnp.float32)[:, :, None, :]
    grouped_table = neighbours.reshape(N_PLANE, SLOTS, 8)
    grouped_mask = mask_f.reshape(N_PLANE, SLOTS, DEPTH, 1, CELLS)
    full_shape = hidden.shape
    for block_id in range(BLOCKS):
        branch = hidden
        for layer_id in range(3):
            strip_pool = strips(branch.reshape(full_shape[:-1] + (TILE, TILE)), 1)
            weight = plane_weight[block_id, layer_id]
            offsets = plane_bias[block_id, layer_id][:, None]

            def layer_group(operands):
                group_tiles, group_table, group_mask = operands
                padded = surround(group_tiles.reshape(group_tiles.shape[:-1] + (TILE, TILE)), group_table, strip_pool, 1)
                summed = plane_conv(padded, weight)
                return (group_mask * jax.nn.silu(summed + offsets)).astype(jnp.bfloat16)

            branch = lax.map(layer_group, (branch.reshape((N_PLANE, SLOTS) + full_shape[1:]), grouped_table, grouped_mask)).reshape(full_shape)
        padded_z = jnp.pad(branch, ((0, 0), (1, 1), (0, 0), (0, 0)))
        weight_d = depth_weight[block_id].astype(jnp.float32)
        offsets_d = depth_bias[block_id][:, None]

        def depth_group(operands):
            group_pad, group_mask, group_hidden = operands
            stacked = jnp.concatenate([group_pad[:, :-2], group_pad[:, 1:-1], group_pad[:, 2:]], axis=2)
            summed = jnp.einsum("ok,nskq->nsoq", weight_d, stacked.astype(jnp.float32))
            return (group_hidden.astype(jnp.float32) + group_mask * (summed + offsets_d)).astype(jnp.bfloat16)

        hidden = lax.map(depth_group, (padded_z.reshape((N_PLANE, SLOTS) + padded_z.shape[1:]), grouped_mask, hidden.reshape((N_PLANE, SLOTS) + full_shape[1:]))).reshape(full_shape)
    return hidden
```

```python
import functools
import math

import jax
import jax.numpy as jnp
from jax import lax
from jax.experimental import pallas as pl
from jax.experimental.pallas import tpu as pltpu
from jax.sharding import PartitionSpec as P

F32 = jnp.float32
BF16 = jnp.bfloat16
LANES = 128
BLOCK = 256
FRONT = LANES
AUG = 8
LAYERS = 3


class Geometry:
    def __init__(self, cells, blocks):
        self.tile = math.isqrt(cells)
        self.halo = LAYERS * blocks
        self.side = self.tile + 2 * self.halo
        self.blocks = blocks
        body = -(-self.side * self.side // BLOCK) * BLOCK
        self.body = body
        self.width = FRONT + body + LANES
        self.strip = self.halo * self.tile

    def lane(self, row, col):
        return FRONT + row * self.side + col

    def span(self, margin):
        first = self.lane(margin, margin)
        last = self.lane(self.side - 1 - margin, self.side - 1 - margin)
        return first // LANES * LANES, (last // LANES + 1) * LANES


def whole():
    return pl.BlockSpec(memory_space=pltpu.VMEM)


def scalars():
    return pl.BlockSpec(memory_space=pltpu.SMEM)


def params(mib=20):
    return pltpu.CompilerParams(vmem_limit_bytes=mib << 20)


def cost(flops, moved=1 << 20):
    return pl.CostEstimate(flops=flops, bytes_accessed=moved, transcendentals=0)


def iota(shape, dim):
    return lax.broadcasted_iota(jnp.int32, shape, dim)


def one_hot(condition):
    return jnp.where(condition, 1.0, 0.0).astype(BF16)


def dot(a, b):
    return jnp.dot(a, b, preferred_element_type=F32)


KIND = (0, 0, 0, 2, 3, 1, 1, 1)


def pack_kernel(g, slots, planes, nbr_ref, counts_ref, acts_ref, mask_ref, *refs):
    out_refs, (aug_ref, strip_ref) = refs[:planes], refs[planes:]
    me = lax.axis_index("plane")
    tile, halo = g.tile, g.halo
    cells = tile * tile
    rows = acts_ref.shape[2]
    per_tile = LANES // tile
    half = LANES // 2
    lane = iota((cells, 2 * LANES), 1)
    lane = jnp.where(lane >= LANES + half, lane - half, lane)
    source = iota((cells, 2 * LANES), 0)
    row, col = source // tile, source % tile
    left = one_hot((row * halo + col == lane) & (col < halo))
    right = one_hot((row * halo + col - (tile - halo) == lane) & (col >= tile - halo))
    i, j = iota((LANES, LANES), 0), iota((LANES, LANES), 1)
    low = one_hot(i == j % half)
    high = one_hot(i == half + j % half)
    for a in range(slots):
        alive = a < counts_ref[me]
        aug_ref[a, :rows] = jnp.where(alive, acts_ref[a, 0].astype(F32), 0.0).astype(BF16)
        line = mask_ref[a, 0:1].astype(F32)
        aug_ref[a, rows:] = jnp.where(iota((AUG, cells), 0) == 0, line, 0.0).astype(BF16)
        x = aug_ref[a]
        strip_ref[a, 0, 0] = x[:, :LANES]
        strip_ref[a, 0, 1] = dot(x[:, LANES : 2 * LANES], low).astype(BF16)
        strip_ref[a, 1, 0] = x[:, cells - LANES :]
        strip_ref[a, 1, 1] = dot(x[:, cells - 2 * LANES : cells - LANES], high).astype(BF16)
        for kind, pick in ((2, left), (3, right)):
            both = dot(x, pick).astype(BF16)
            strip_ref[a, kind, 0] = both[:, :LANES]
            strip_ref[a, kind, 1] = both[:, LANES:]
    lower = iota((rows + AUG, LANES), 1) < half
    for k in range(planes):
        peer = partner(me, k, planes, True)
        for a in range(slots):
            kinds = []
            for b in range(slots):
                kind = jnp.int32(0)
                for d in range(8):
                    kind = jnp.where(nbr_ref[a, d] == peer * slots + b, KIND[d], kind)
                kinds.append(kind)
                out_refs[k][slots * a + b] = strip_ref[a, kind, 0]
            out_refs[k][slots * slots + a] = jnp.where(lower, strip_ref[a, kinds[0], 1], strip_ref[a, kinds[1], 1])


def partner(me, k, planes, outgoing):
    if planes & (planes - 1) == 0:
        return me ^ k
    return lax.rem(me + (k if outgoing else planes - k), planes)


def route(me, other, planes):
    if planes & (planes - 1) == 0:
        return me ^ other
    return lax.rem(me - other + planes, planes)


def halo_pieces(g):
    tile, halo, side = g.tile, g.halo, g.side
    pieces = []
    for d in (0, 1, 2, 5, 6, 7):
        first_row = 0 if d < 3 else halo + tile
        cols = {0: (0, halo), 1: (halo, halo + tile), 2: (halo + tile, side)}[d % 3 if d < 3 else (d - 5)]
        blocks = sorted({((first_row + r) * side + c) // BLOCK for r in range(halo) for c in range(*cols)})
        pieces += [(d, n) for n in blocks]
    sides = []
    split = LANES // halo
    for part in (0, 1):
        blocks = set()
        for r in range(tile):
            for c in range(halo):
                if (r * halo + c >= LANES) == bool(part):
                    blocks.add(((halo + r) * side + c) // BLOCK)
                    blocks.add(((halo + r) * side + halo + tile + c) // BLOCK)
        sides += [(part, n) for n in sorted(blocks)]
    return pieces, sides


def cell_of(e, g):
    return e // g.tile, e % g.tile


def strip_entry(lane, b, half):
    rest = lane - LANES
    ours = (rest >= b * half) & (rest < (b + 1) * half)
    return jnp.where(lane < LANES, lane, jnp.where(ours, LANES + rest - b * half, -10000))


def own_band(g):
    pairs = set()
    for r in range(g.tile):
        for c in range(g.tile):
            pairs.add(((r * g.tile + c) // BLOCK, ((r + g.halo) * g.side + c + g.halo) // BLOCK))
    return sorted(pairs)


def prepare_kernel(g, slots, nbr_ref, counts_ref, acts_ref, mask_ref, own_ref, pick_ref, keep_ref, aug_ref):
    me = lax.axis_index("plane")
    tile, halo, side = g.tile, g.halo, g.side
    cells = tile * tile
    rows = acts_ref.shape[2]
    half = LANES // 2
    for a in range(slots):
        alive = a < counts_ref[me]
        aug_ref[a, :rows] = jnp.where(alive, acts_ref[a, 0].astype(F32), 0.0).astype(BF16)
        line = mask_ref[a, 0:1].astype(F32)
        aug_ref[a, rows:] = jnp.where(iota((AUG, cells), 0) == 0, line, 0.0).astype(BF16)
    src = iota((BLOCK, BLOCK), 0)
    dst = iota((BLOCK, BLOCK), 1)
    pairs = own_band(g)
    for n in range(g.body // BLOCK):
        total = [jnp.zeros((rows + AUG, BLOCK), F32) for _ in range(slots)]
        for k in [k for k, m in pairs if m == n]:
            cell = src + k * BLOCK
            where = (cell // tile + halo) * side + cell % tile + halo
            move = one_hot(where == dst + n * BLOCK)
            for a in range(slots):
                total[a] += dot(aug_ref[a, :, k * BLOCK : (k + 1) * BLOCK], move)
        for a in range(slots):
            own_ref[a, :, n * BLOCK : (n + 1) * BLOCK] = total[a].astype(BF16)
    pieces, sides = halo_pieces(g)
    at = 0
    for d, n in pieces:
        for b in range(slots):
            e = strip_entry(src, b, half)
            if d < 3:
                lead = g.strip - LANES
                e = jnp.where(src < LANES, src + lead, e - LANES)
                row, col, base = e // tile, e % tile, 0
            else:
                row, col, base = e // tile, e % tile, halo + tile
            kind = d if d < 3 else d - 5
            if kind == 0:
                good, shift = col >= tile - halo, halo - tile
            elif kind == 1:
                good, shift = col >= 0, halo
            else:
                good, shift = col < halo, halo + tile
            where = (base + row) * side + col + shift
            pick_ref[at] = one_hot((where == dst + n * BLOCK) & good & (e >= 0))
            at += 1
    for part, n in sides:
        for b in range(slots):
            lane = jnp.where(src < LANES, src, src - LANES) + part * LANES
            e = strip_entry(lane, b, half)
            row, col = e // halo, e % halo
            where = (halo + row) * side + col + jnp.where(src < LANES, 0, halo + tile)
            pick_ref[at] = one_hot((where == dst + n * BLOCK) & (e >= 0))
            at += 1
    start, _ = g.span(halo)
    for m, (n, k) in enumerate(keep_band(g)):
        cell = dst + n * BLOCK
        where = FRONT + (cell // tile + halo) * side + cell % tile + halo - start
        keep_ref[m] = one_hot(where == src + k * BLOCK)


def keep_band(g):
    start, _ = g.span(g.halo)
    pairs = set()
    for r in range(g.tile):
        for c in range(g.tile):
            pairs.add(((r * g.tile + c) // BLOCK, (g.lane(r + g.halo, c + g.halo) - start) // BLOCK))
    return sorted(pairs)


def conv(g, x_ref, y_ref, stack_ref, weight, bias, mask_ref, start, stop):
    channels = weight.shape[0]
    width = stop - start
    for row in range(3):
        for col in range(3):
            tap = row * 3 + col
            off = start + (row - 1) * g.side + col - 1
            stack_ref[tap * channels : (tap + 1) * channels, :width] = x_ref[:, off : off + width]
    for at in range(0, width, BLOCK):
        size = min(BLOCK, width - at)
        total = dot(weight, stack_ref[:, at : at + size])
        half = 0.5 * (total + bias)
        out = (half + half * jnp.tanh(half)) * mask_ref[0:1, start + at : start + at + size]
        y_ref[:, start + at : start + at + size] = out.astype(BF16)


def branch(g, block, bufs, stack_ref, weight_ref, bias_ref, mask_ref):
    margin = LAYERS * block + 1
    for layer in range(LAYERS):
        start, stop = g.span(margin + layer)
        conv(
            g,
            bufs[layer % 2],
            bufs[(layer + 1) % 2],
            stack_ref,
            weight_ref[block, layer],
            bias_ref[block, layer],
            mask_ref,
            start,
            stop,
        )
    return bufs[LAYERS % 2]


def first_kernel(g, slots, planes, nbr_ref, own_ref, pick_ref, weight_ref, bias_ref, *refs):
    messages = refs[:planes]
    branch_ref, hidden_ref, mask_ref, pool_ref, x_ref, y_ref, stack_ref = refs[planes:]
    me = lax.axis_index("plane")
    channels = weight_ref.shape[2]
    for k in range(planes):
        pool_ref[k] = messages[k][...]
    pieces, sides = halo_pieces(g)
    start, stop = g.span(LAYERS)
    for b in range(slots):

        def fetch(d):
            source = nbr_ref[b, d]
            safe = jnp.maximum(source, 0)
            k = route(me, safe // slots, planes)
            a = safe % slots
            ok = source >= 0
            main = pool_ref[k, slots * a + b]
            rest = pool_ref[k, slots * slots + a]
            main = jnp.where(ok, main.astype(F32), 0.0).astype(BF16)
            rest = jnp.where(ok, rest.astype(F32), 0.0).astype(BF16)
            return main, rest

        strips = {d: fetch(d) for d in range(8)}
        lines = {d: jnp.concatenate(strips[d], axis=1) for d in (0, 1, 2, 5, 6, 7)}
        walls = [jnp.concatenate([strips[3][part], strips[4][part]], axis=1) for part in (0, 1)]
        for n in range(g.body // BLOCK):
            total = own_ref[b, :, n * BLOCK : (n + 1) * BLOCK].astype(F32)
            for at, (d, m) in enumerate(pieces):
                if m == n:
                    total += dot(lines[d], pick_ref[at * slots + b])
            for at, (part, m) in enumerate(sides):
                if m == n:
                    total += dot(walls[part], pick_ref[(len(pieces) + at) * slots + b])
            lanes = slice(FRONT + n * BLOCK, FRONT + (n + 1) * BLOCK)
            x_ref[b, :, lanes] = total[:channels].astype(BF16)
            mask_ref[b, :, lanes] = total[channels:]
        x_ref[b, :, :FRONT] = jnp.zeros((channels, FRONT), BF16)
        x_ref[b, :, FRONT + g.body :] = jnp.zeros((channels, LANES), BF16)
        y_ref[b] = jnp.zeros(y_ref.shape[1:], BF16)
        hidden_ref[b] = x_ref[b, :, start:stop]
        out = branch(g, 0, (x_ref.at[b], y_ref.at[b]), stack_ref.at[b], weight_ref, bias_ref, mask_ref.at[b])
        branch_ref[b] = out[:, start:stop]


def depth_sum(block, bias_ref, weight_ref, pair_tap, other_tap, own, pair, other):
    total = dot(weight_ref[block, 1], own)
    total += dot(weight_ref[block, pair_tap], pair)
    total += dot(weight_ref[block, other_tap], other)
    return total + bias_ref[block]


def depth_taps():
    odd = lax.rem(lax.axis_index("depth"), 2)
    return 2 - 2 * odd, 2 * odd


def second_kernel(
    g,
    slots,
    own_ref,
    pair_ref,
    other_ref,
    hidden_ref,
    mask_ref,
    keep_ref,
    weight_ref,
    bias_ref,
    dweight_ref,
    dbias_ref,
    branch_ref,
    kept_ref,
    x_ref,
    y_ref,
    stack_ref,
):
    pair_tap, other_tap = depth_taps()
    start, stop = g.span(LAYERS)
    inner, outer = g.span(g.halo)
    band = keep_band(g)
    cells = g.tile * g.tile

    def keep(buf, ref):
        for n in range(cells // BLOCK):
            total = None
            for m, (i, k) in enumerate(band):
                if i == n:
                    lo = inner + k * BLOCK
                    term = dot(buf[:, lo : lo + BLOCK], keep_ref[m])
                    total = term if total is None else total + term
            ref[:, n * BLOCK : (n + 1) * BLOCK] = total.astype(BF16)

    for b in range(slots):
        x_ref[b, :, :start] = jnp.zeros((x_ref.shape[1], start), BF16)
        x_ref[b, :, stop:] = jnp.zeros((x_ref.shape[1], x_ref.shape[2] - stop), BF16)
        y_ref[b] = jnp.zeros(y_ref.shape[1:], BF16)
        for at in range(0, stop - start, BLOCK):
            size = min(BLOCK, stop - start - at)
            piece = slice(at, at + size)
            summed = depth_sum(
                0, dbias_ref, dweight_ref, pair_tap, other_tap, own_ref[b, :, piece], pair_ref[b, :, piece], other_ref[b, :, piece]
            )
            lanes = slice(start + at, start + at + size)
            x_ref[b, :, lanes] = (hidden_ref[b, :, piece].astype(F32) + mask_ref[b, 0:1, lanes] * summed).astype(BF16)
        keep(x_ref.at[b], kept_ref.at[b])
        out = branch(g, 1, (x_ref.at[b], y_ref.at[b]), stack_ref.at[b], weight_ref, bias_ref, mask_ref.at[b])
        keep(out, branch_ref.at[b])


def last_kernel(slots, block, own_ref, pair_ref, other_ref, kept_ref, mask_ref, dweight_ref, dbias_ref, out_ref):
    pair_tap, other_tap = depth_taps()
    for b in range(slots):
        summed = depth_sum(block, dbias_ref, dweight_ref, pair_tap, other_tap, own_ref[b], pair_ref[b], other_ref[b])
        mask = mask_ref[b, 0:1].astype(F32)
        out_ref[b, 0] = (kept_ref[b].astype(F32) + mask * summed).astype(BF16)


def neighbours_in_depth(x):
    count = lax.axis_size("depth")

    def swap(first):
        perm = []
        for i in range(first, count - 1, 2):
            perm += [(i, i + 1), (i + 1, i)]
        return lax.ppermute(x, "depth", perm)

    other = swap(1)
    pair = swap(0)
    return pair, other


def shards(
    activations, plane_weight, plane_bias, depth_weight, depth_bias, counts, neighbours, voxel_mask
):
    slots, sections, channels, cells = activations.shape
    blocks = plane_weight.shape[0]
    planes = lax.axis_size("plane")
    assert slots == 2 and sections == 1 and blocks == 2
    g = Geometry(cells, blocks)
    bias = plane_bias[..., None]
    dbias = depth_bias[..., None]
    dweight = depth_weight.reshape(blocks, channels, 3, channels).transpose(0, 2, 1, 3)
    rows = channels + AUG
    message = jax.ShapeDtypeStruct((slots * slots + slots, rows, LANES), BF16)
    packed = pl.pallas_call(
        functools.partial(pack_kernel, g, slots, planes),
        out_shape=[message] * planes,
        in_specs=[scalars(), scalars(), whole(), whole()],
        out_specs=[whole()] * planes,
        scratch_shapes=[
            pltpu.VMEM((slots, rows, cells), BF16),
            pltpu.VMEM((slots, 4, 2, rows, LANES), BF16),
        ],
        compiler_params=params(),
        cost_estimate=cost(1 << 28),
        name="pack",
    )(neighbours, counts, activations, voxel_mask)
    received = [packed[0]] + [None] * (planes - 1)
    for k in reversed(range(1, planes)):
        if planes & (planes - 1) == 0:
            perm = [(i, i ^ k) for i in range(planes)]
        else:
            perm = [(i, (i + k) % planes) for i in range(planes)]
        received[k] = lax.ppermute(packed[k], "plane", perm)

    pieces, sides = halo_pieces(g)
    own, pick, keep = pl.pallas_call(
        functools.partial(prepare_kernel, g, slots),
        out_shape=[
            jax.ShapeDtypeStruct((slots, rows, g.body), BF16),
            jax.ShapeDtypeStruct(((len(pieces) + len(sides)) * slots, BLOCK, BLOCK), BF16),
            jax.ShapeDtypeStruct((len(keep_band(g)), BLOCK, BLOCK), BF16),
        ],
        in_specs=[scalars(), scalars(), whole(), whole()],
        out_specs=[whole()] * 3,
        scratch_shapes=[pltpu.VMEM((slots, rows, cells), BF16)],
        compiler_params=params(),
        cost_estimate=cost(1 << 29),
        name="prepare",
    )(neighbours, counts, activations, voxel_mask)

    start, stop = g.span(LAYERS)
    work = [
        pltpu.VMEM((slots, channels, g.width), BF16),
        pltpu.VMEM((slots, channels, g.width), BF16),
        pltpu.VMEM((slots, 9 * channels, g.body), BF16),
    ]
    wide = jax.ShapeDtypeStruct((slots, channels, stop - start), BF16)
    branch0, hidden0, mask = pl.pallas_call(
        functools.partial(first_kernel, g, slots, planes),
        out_shape=[wide, wide, jax.ShapeDtypeStruct((slots, AUG, g.width), F32)],
        in_specs=[scalars()] + [whole()] * (4 + planes),
        out_specs=[whole()] * 3,
        scratch_shapes=[pltpu.VMEM((planes,) + message.shape, BF16)] + work,
        compiler_params=params(30),
        cost_estimate=cost(1 << 31),
        name="first",
    )(neighbours, own, pick, plane_weight, bias, *received)
    pair, other = neighbours_in_depth(branch0)
    narrow = jax.ShapeDtypeStruct((slots, channels, cells), BF16)
    branch1, kept = pl.pallas_call(
        functools.partial(second_kernel, g, slots),
        out_shape=[narrow, narrow],
        in_specs=[whole()] * 10,
        out_specs=[whole()] * 2,
        scratch_shapes=work,
        compiler_params=params(30),
        cost_estimate=cost(1 << 31),
        name="second",
    )(branch0, pair, other, hidden0, mask, keep, plane_weight, bias, dweight, dbias)
    pair, other = neighbours_in_depth(branch1)
    return pl.pallas_call(
        functools.partial(last_kernel, slots, blocks - 1),
        out_shape=jax.ShapeDtypeStruct(activations.shape, BF16),
        in_specs=[whole()] * 7,
        out_specs=whole(),
        compiler_params=params(),
        cost_estimate=cost(1 << 26),
        name="last",
    )(branch1, pair, other, kept, voxel_mask, dweight, dbias)


def solution(mesh):
    in_specs = (
        P("plane", "depth", None, None),
        P(),
        P(),
        P(),
        P(),
        P(),
        P("plane", None),
        P("plane", "depth", None),
    )
    out_specs = P("plane", "depth", None, None)
    return jax.shard_map(shards, mesh=mesh, in_specs=in_specs, out_specs=out_specs, check_vma=False)
```

```python
import functools
import math

import jax
import jax.numpy as jnp
from jax import lax
from jax.experimental import pallas as pl
from jax.experimental.pallas import tpu as pltpu
from jax.sharding import PartitionSpec as P


F32 = jnp.float32
BF16 = jnp.bfloat16
LANES = 128
BLOCK = 256
FRONT = 2 * LANES
AUG = 8
LAYERS = 3


class Geometry:
    def __init__(self, cells, blocks):
        self.tile = math.isqrt(cells)
        self.halo = LAYERS * blocks
        self.side = self.tile + 2 * self.halo
        self.blocks = blocks
        body = -(-self.side * self.side // BLOCK) * BLOCK
        self.body = body
        self.width = FRONT + body + LANES
        self.strip = self.halo * self.tile

    def lane(self, row, col):
        return FRONT + row * self.side + col

    def span(self, margin):
        first = self.lane(margin, margin)
        last = self.lane(self.side - 1 - margin, self.side - 1 - margin)
        return first // LANES * LANES, (last // LANES + 1) * LANES


def whole():
    return pl.BlockSpec(memory_space=pltpu.VMEM)


def hbm():
    return pl.BlockSpec(memory_space=pltpu.HBM)


def keep_in_hbm(x):
    return pltpu.with_memory_space_constraint(x, pltpu.HBM)


def params(mib=8):
    return pltpu.CompilerParams(vmem_limit_bytes=mib << 20)


def cost(flops, moved=1 << 20):
    return pl.CostEstimate(flops=flops, bytes_accessed=moved, transcendentals=0)


def iota(shape, dim):
    return lax.broadcasted_iota(jnp.int32, shape, dim)


def one_hot(condition):
    return jnp.where(condition, 1.0, 0.0).astype(BF16)


def dot(a, b):
    return jnp.dot(a, b, preferred_element_type=F32)


KIND = (0, 0, 0, 2, 3, 1, 1, 1)


def pack_kernel(g, slots, planes, nbr_hbm, counts_hbm, acts_hbm, mask_hbm, *refs):
    out_refs, (aug_ref, strip_ref, acts_ref, mask_ref, nbr_ref, counts_ref, sems) = refs[:planes], refs[planes:]
    copies = [
        pltpu.make_async_copy(source, target, sems.at[at])
        for at, (source, target) in enumerate(
            ((acts_hbm, acts_ref), (mask_hbm, mask_ref), (nbr_hbm, nbr_ref), (counts_hbm, counts_ref))
        )
    ]
    for copy in copies:
        copy.start()
    me = lax.axis_index("plane")
    tile, halo = g.tile, g.halo
    cells = tile * tile
    rows = acts_ref.shape[2]
    half = LANES // 2
    lane = iota((cells, 2 * LANES), 1)
    lane = jnp.where(lane >= LANES + half, lane - half, lane)
    source = iota((cells, 2 * LANES), 0)
    row, col = source // tile, source % tile
    left = one_hot((row * halo + col == lane) & (col < halo))
    right = one_hot((row * halo + col - (tile - halo) == lane) & (col >= tile - halo))
    i, j = iota((LANES, LANES), 0), iota((LANES, LANES), 1)
    low = one_hot(i == j % half)
    high = one_hot(i == half + j % half)
    for copy in copies:
        copy.wait()
    for a in range(slots):
        alive = a < counts_ref[me]
        aug_ref[a, :rows] = jnp.where(alive, acts_ref[a, 0].astype(F32), 0.0).astype(BF16)
        line = mask_ref[a, 0:1].astype(F32)
        aug_ref[a, rows:] = jnp.where(iota((AUG, cells), 0) == 0, line, 0.0).astype(BF16)
        x = aug_ref[a]
        strip_ref[a, 0, 0] = x[:, :LANES]
        strip_ref[a, 0, 1] = dot(x[:, LANES : 2 * LANES], low).astype(BF16)
        strip_ref[a, 1, 0] = x[:, cells - LANES :]
        strip_ref[a, 1, 1] = dot(x[:, cells - 2 * LANES : cells - LANES], high).astype(BF16)
        for kind, pick in ((2, left), (3, right)):
            both = dot(x, pick).astype(BF16)
            strip_ref[a, kind, 0] = both[:, :LANES]
            strip_ref[a, kind, 1] = both[:, LANES:]
    lower = iota((rows + AUG, LANES), 1) < half
    for k in range(planes):
        peer = partner(me, k, planes, True)
        for a in range(slots):
            kinds = []
            for b in range(slots):
                kind = jnp.int32(0)
                for d in range(8):
                    kind = jnp.where(nbr_ref[a, d] == peer * slots + b, KIND[d], kind)
                kinds.append(kind)
                out_refs[k][slots * a + b] = strip_ref[a, kind, 0]
            out_refs[k][slots * slots + a] = jnp.where(lower, strip_ref[a, kinds[0], 1], strip_ref[a, kinds[1], 1])


def partner(me, k, planes, outgoing):
    if planes & (planes - 1) == 0:
        return me ^ k
    return lax.rem(me + (k if outgoing else planes - k), planes)


def route(me, other, planes):
    if planes & (planes - 1) == 0:
        return me ^ other
    return lax.rem(me - other + planes, planes)


def halo_pieces(g):
    tile, halo, side = g.tile, g.halo, g.side
    pieces = []
    for d in (0, 1, 2, 5, 6, 7):
        first_row = 0 if d < 3 else halo + tile
        cols = {0: (0, halo), 1: (halo, halo + tile), 2: (halo + tile, side)}[d % 3 if d < 3 else (d - 5)]
        blocks = sorted({((first_row + r) * side + c) // BLOCK for r in range(halo) for c in range(*cols)})
        pieces += [(d, n) for n in blocks]
    sides = []
    for part in (0, 1):
        blocks = set()
        for r in range(tile):
            for c in range(halo):
                if (r * halo + c >= LANES) == bool(part):
                    blocks.add(((halo + r) * side + c) // BLOCK)
                    blocks.add(((halo + r) * side + halo + tile + c) // BLOCK)
        sides += [(part, n) for n in sorted(blocks)]
    return pieces, sides


def strip_entry(lane, b, half):
    rest = lane - LANES
    ours = (rest >= b * half) & (rest < (b + 1) * half)
    return jnp.where(lane < LANES, lane, jnp.where(ours, LANES + rest - b * half, -10000))


def own_band(g):
    pairs = set()
    for r in range(g.tile):
        for c in range(g.tile):
            pairs.add(((r * g.tile + c) // BLOCK, ((r + g.halo) * g.side + c + g.halo) // BLOCK))
    return sorted(pairs)


def prepare_kernel(
    g,
    slots,
    aug_ref,
    nbr_hbm,
    weight_hbm,
    bias_hbm,
    dweight_hbm,
    dbias_hbm,
    own_ref,
    pick_ref,
    keep_ref,
    table_ref,
    weight_ref,
    bias_ref,
    dweight_ref,
    raw_weight_ref,
    raw_bias_ref,
    raw_dweight_ref,
    raw_dbias_ref,
    sems,
):
    copies = [
        pltpu.make_async_copy(source, target, sems.at[at])
        for at, (source, target) in enumerate(
            (
                (weight_hbm, raw_weight_ref),
                (bias_hbm, raw_bias_ref),
                (dweight_hbm, raw_dweight_ref),
                (dbias_hbm, raw_dbias_ref),
                (nbr_hbm, table_ref),
            )
        )
    ]
    for copy in copies:
        copy.start()
    tile, halo, side = g.tile, g.halo, g.side
    rows = aug_ref.shape[1] - AUG
    half = LANES // 2
    src = iota((BLOCK, BLOCK), 0)
    dst = iota((BLOCK, BLOCK), 1)
    pairs = own_band(g)
    for n in range(g.body // BLOCK):
        total = [jnp.zeros((rows + AUG, BLOCK), F32) for _ in range(slots)]
        for k in [k for k, m in pairs if m == n]:
            cell = src + k * BLOCK
            where = (cell // tile + halo) * side + cell % tile + halo
            move = one_hot(where == dst + n * BLOCK)
            for a in range(slots):
                total[a] += dot(aug_ref[a, :, k * BLOCK : (k + 1) * BLOCK], move)
        for a in range(slots):
            own_ref[a, :, n * BLOCK : (n + 1) * BLOCK] = total[a].astype(BF16)
    pieces, sides = halo_pieces(g)
    at = 0
    for d, n in pieces:
        for b in range(slots):
            e = strip_entry(src, b, half)
            if d < 3:
                lead = g.strip - LANES
                e = jnp.where(src < LANES, src + lead, e - LANES)
                row, col, base = e // tile, e % tile, 0
            else:
                row, col, base = e // tile, e % tile, halo + tile
            kind = d if d < 3 else d - 5
            if kind == 0:
                good, shift = col >= tile - halo, halo - tile
            elif kind == 1:
                good, shift = col >= 0, halo
            else:
                good, shift = col < halo, halo + tile
            where = (base + row) * side + col + shift
            pick_ref[at] = one_hot((where == dst + n * BLOCK) & good & (e >= 0))
            at += 1
    for part, n in sides:
        for b in range(slots):
            lane = jnp.where(src < LANES, src, src - LANES) + part * LANES
            e = strip_entry(lane, b, half)
            row, col = e // halo, e % halo
            where = (halo + row) * side + col + jnp.where(src < LANES, 0, halo + tile)
            pick_ref[at] = one_hot((where == dst + n * BLOCK) & (e >= 0))
            at += 1
    start, _ = g.span(halo)
    for m, (n, k) in enumerate(keep_band(g)):
        cell = dst + n * BLOCK
        where = FRONT + (cell // tile + halo) * side + cell % tile + halo - start
        keep_ref[m] = one_hot(where == src + k * BLOCK)
    for copy in copies:
        copy.wait()
    odd = lax.rem(lax.axis_index("depth"), 2)
    diagonal = iota((rows, rows), 0) == iota((rows, rows), 1)

    def column(line):
        return jnp.sum(jnp.where(diagonal, line, 0.0), axis=1, keepdims=True)

    for block in range(g.blocks):
        for layer in range(LAYERS):
            for at, row in enumerate((1, 0, 2)):
                piece = raw_weight_ref[block, layer, :, 3 * row * rows : 3 * (row + 1) * rows]
                weight_ref[block, layer, at * rows : (at + 1) * rows] = (0.5 * piece.astype(F32)).astype(BF16)
            bias_ref[block, layer] = 0.5 * column(raw_bias_ref[layer, block : block + 1])
        bias_ref[block, LAYERS] = column(raw_dbias_ref[block : block + 1])
        taps = [raw_dweight_ref[block, :, tap * rows : (tap + 1) * rows].astype(F32) for tap in range(3)]
        dweight_ref[block, 0] = jnp.where(odd == 1, taps[0], taps[2]).astype(BF16)
        dweight_ref[block, 1] = taps[1].astype(BF16)
        dweight_ref[block, 2] = jnp.where(odd == 1, taps[2], taps[0]).astype(BF16)


def keep_band(g):
    start, _ = g.span(g.halo)
    pairs = set()
    for r in range(g.tile):
        for c in range(g.tile):
            pairs.add(((r * g.tile + c) // BLOCK, (g.lane(r + g.halo, c + g.halo) - start) // BLOCK))
    return sorted(pairs)


def conv(g, margin, x_ref, y_ref, stack_ref, middle_ref, outer_ref, weight, bias, mask_ref):
    channels = x_ref.shape[0]
    low, high = g.span(margin - 1)
    start, stop = g.span(margin)
    for col in range(3):
        stack_ref[col * channels : (col + 1) * channels, low:high] = x_ref[:, low + col - 1 : high + col - 1]
    for at in range(low, high, BLOCK):
        lanes = slice(at, min(at + BLOCK, high))
        sums = dot(weight, stack_ref[:, lanes])
        middle_ref[:, lanes] = sums[:channels]
        outer_ref[:, lanes] = sums[channels:]
    for at in range(start, stop, BLOCK):
        end = min(at + BLOCK, stop)
        above = outer_ref[:channels, at - g.side : end - g.side]
        below = outer_ref[channels:, at + g.side : end + g.side]
        half = middle_ref[:, at:end] + bias + above + below
        out = (half + half * jnp.tanh(half)) * mask_ref[0:1, at:end]
        y_ref[:, at:end] = out.astype(BF16)


def branch(g, block, bufs, work, weight_ref, bias_ref, mask_ref):
    for layer in range(LAYERS):
        margin = LAYERS * block + 1 + layer
        source, target = bufs[layer % 2], bufs[(layer + 1) % 2]
        conv(g, margin, source, target, *work, weight_ref[block, layer], bias_ref[block, layer], mask_ref)
    return bufs[LAYERS % 2]


def first_kernel(g, slots, planes, b, table_ref, own_ref, pick_ref, weight_ref, bias_ref, *refs):
    messages = refs[:planes]
    branch_ref, hidden_ref, mask_ref, pool_ref, x_ref, y_ref, *work = refs[planes:]
    me = lax.axis_index("plane")
    channels = weight_ref.shape[2] // 3
    table = table_ref[b : b + 1].astype(F32)
    for k in range(planes):
        for a in range(slots):
            pool_ref[k, a, 0] = messages[k][slots * a + b]
            pool_ref[k, a, 1] = messages[k][slots * slots + a]
    pieces, sides = halo_pieces(g)
    start, stop = g.span(LAYERS)

    def fetch(d):
        source = jnp.sum(jnp.where(iota(table.shape, 1) == d, table, 0.0)).astype(jnp.int32)
        safe = jnp.maximum(source, 0)
        k = route(me, safe // slots, planes)
        a = safe % slots
        ok = source >= 0
        main = pool_ref[k, a, 0]
        rest = pool_ref[k, a, 1]
        main = jnp.where(ok, main.astype(F32), 0.0).astype(BF16)
        rest = jnp.where(ok, rest.astype(F32), 0.0).astype(BF16)
        return main, rest

    strips = {d: fetch(d) for d in range(8)}
    lines = {d: jnp.concatenate(strips[d], axis=1) for d in (0, 1, 2, 5, 6, 7)}
    walls = [jnp.concatenate([strips[3][part], strips[4][part]], axis=1) for part in (0, 1)]
    for n in range(g.body // BLOCK):
        total = own_ref[b, :, n * BLOCK : (n + 1) * BLOCK].astype(F32)
        for at, (d, m) in enumerate(pieces):
            if m == n:
                total += dot(lines[d], pick_ref[at * slots + b])
        for at, (part, m) in enumerate(sides):
            if m == n:
                total += dot(walls[part], pick_ref[(len(pieces) + at) * slots + b])
        lanes = slice(FRONT + n * BLOCK, FRONT + (n + 1) * BLOCK)
        x_ref[:, lanes] = total[:channels].astype(BF16)
        mask_ref[:, lanes] = total[channels:]
    x_ref[:, :FRONT] = jnp.zeros((channels, FRONT), BF16)
    x_ref[:, FRONT + g.body :] = jnp.zeros((channels, LANES), BF16)
    y_ref[...] = jnp.zeros(y_ref.shape, BF16)
    hidden_ref[...] = x_ref[:, start:stop]
    out = branch(g, 0, (x_ref, y_ref), work, weight_ref, bias_ref, mask_ref)
    branch_ref[...] = out[:, start:stop]


def depth_sum(block, bias_ref, weight_ref, own, pair, other):
    total = dot(weight_ref[block, 1], own)
    total += dot(weight_ref[block, 0], pair)
    total += dot(weight_ref[block, 2], other)
    return total + bias_ref[block, LAYERS]


def second_kernel(
    g,
    own_ref,
    pair_ref,
    other_ref,
    hidden_ref,
    mask_ref,
    keep_ref,
    weight_ref,
    bias_ref,
    dweight_ref,
    branch_ref,
    kept_ref,
    x_ref,
    y_ref,
    *work,
):
    start, stop = g.span(LAYERS)
    inner, _ = g.span(g.halo)
    band = keep_band(g)
    cells = g.tile * g.tile

    def keep(buf, ref):
        for n in range(cells // BLOCK):
            total = None
            for m, (i, k) in enumerate(band):
                if i == n:
                    lo = inner + k * BLOCK
                    term = dot(buf[:, lo : lo + BLOCK], keep_ref[m])
                    total = term if total is None else total + term
            ref[:, n * BLOCK : (n + 1) * BLOCK] = total.astype(BF16)

    x_ref[:, :start] = jnp.zeros((x_ref.shape[0], start), BF16)
    x_ref[:, stop:] = jnp.zeros((x_ref.shape[0], x_ref.shape[1] - stop), BF16)
    y_ref[...] = jnp.zeros(y_ref.shape, BF16)
    for at in range(0, stop - start, BLOCK):
        size = min(BLOCK, stop - start - at)
        piece = slice(at, at + size)
        summed = depth_sum(0, bias_ref, dweight_ref, own_ref[:, piece], pair_ref[:, piece], other_ref[:, piece])
        lanes = slice(start + at, start + at + size)
        x_ref[:, lanes] = (hidden_ref[:, piece].astype(F32) + mask_ref[0:1, lanes] * summed).astype(BF16)
    keep(x_ref, kept_ref)
    out = branch(g, 1, (x_ref, y_ref), work, weight_ref, bias_ref, mask_ref)
    keep(out, branch_ref)


def last_kernel(block, b, own_ref, pair_ref, other_ref, kept_ref, mask_ref, bias_ref, dweight_ref, *refs):
    out_ref = refs[-1]
    channels = out_ref.shape[2]
    summed = depth_sum(block, bias_ref, dweight_ref, own_ref[...], pair_ref[...], other_ref[...])
    mask = mask_ref[b, channels : channels + 1].astype(F32)
    out_ref[0, 0] = (kept_ref[...].astype(F32) + mask * summed).astype(BF16)


def neighbours_in_depth(x):
    count = lax.axis_size("depth")

    def swap(first):
        perm = []
        for i in range(first, count - 1, 2):
            perm += [(i, i + 1), (i + 1, i)]
        return lax.ppermute(x, "depth", perm)

    other = swap(1)
    pair = swap(0)
    return pair, other


def shards(
    activations, plane_weight, plane_bias, depth_weight, depth_bias, counts, neighbours, voxel_mask
):
    slots, sections, channels, cells = activations.shape
    blocks = plane_weight.shape[0]
    planes = lax.axis_size("plane")
    assert slots == 2 and sections == 1 and blocks == 2
    g = Geometry(cells, blocks)
    rows = channels + AUG
    message = jax.ShapeDtypeStruct((slots * slots + slots, rows, LANES), BF16)
    aug_shape = jax.ShapeDtypeStruct((slots, rows, cells), BF16)
    *packed, aug = pl.pallas_call(
        functools.partial(pack_kernel, g, slots, planes),
        out_shape=[message] * planes + [aug_shape],
        in_specs=[hbm()] * 4,
        out_specs=[whole()] * (planes + 1),
        scratch_shapes=[
            pltpu.VMEM((slots, 4, 2, rows, LANES), BF16),
            pltpu.VMEM(activations.shape, BF16),
            pltpu.VMEM(voxel_mask.shape, jnp.int32),
            pltpu.SMEM(neighbours.shape, jnp.int32),
            pltpu.SMEM(counts.shape, jnp.int32),
            pltpu.SemaphoreType.DMA((4,)),
        ],
        compiler_params=params(),
        cost_estimate=cost(1 << 28),
        name="pack",
    )(*map(keep_in_hbm, (neighbours, counts, activations, voxel_mask)))
    received = [packed[0]] + [None] * (planes - 1)
    for k in reversed(range(1, planes)):
        if planes & (planes - 1) == 0:
            perm = [(i, i ^ k) for i in range(planes)]
        else:
            perm = [(i, (i + k) % planes) for i in range(planes)]
        received[k] = lax.ppermute(packed[k], "plane", perm)

    pieces, sides = halo_pieces(g)
    own, pick, keep, table, weight, bias, dweight = pl.pallas_call(
        functools.partial(prepare_kernel, g, slots),
        out_shape=[
            jax.ShapeDtypeStruct((slots, rows, g.body), BF16),
            jax.ShapeDtypeStruct(((len(pieces) + len(sides)) * slots, BLOCK, BLOCK), BF16),
            jax.ShapeDtypeStruct((len(keep_band(g)), BLOCK, BLOCK), BF16),
            jax.ShapeDtypeStruct(neighbours.shape, jnp.int32),
            jax.ShapeDtypeStruct((blocks, LAYERS, 3 * channels, 3 * channels), BF16),
            jax.ShapeDtypeStruct((blocks, LAYERS + 1, channels, 1), F32),
            jax.ShapeDtypeStruct((blocks, 3, channels, channels), BF16),
        ],
        in_specs=[whole()] + [hbm()] * 5,
        out_specs=[whole()] * 7,
        scratch_shapes=[
            pltpu.VMEM(plane_weight.shape, BF16),
            pltpu.VMEM((LAYERS, blocks, channels), F32),
            pltpu.VMEM(depth_weight.shape, BF16),
            pltpu.VMEM(depth_bias.shape, F32),
            pltpu.SemaphoreType.DMA((5,)),
        ],
        compiler_params=params(),
        cost_estimate=cost(1 << 29),
        name="prepare",
    )(aug, *map(keep_in_hbm, (neighbours, plane_weight, plane_bias.swapaxes(0, 1), depth_weight, depth_bias)))

    start, stop = g.span(LAYERS)
    work = [
        pltpu.VMEM((channels, g.width), BF16),
        pltpu.VMEM((channels, g.width), BF16),
        pltpu.VMEM((3 * channels, g.width), BF16),
        pltpu.VMEM((channels, g.width), F32),
        pltpu.VMEM((2 * channels, g.width), F32),
    ]
    wide = jax.ShapeDtypeStruct((channels, stop - start), BF16)
    narrow = jax.ShapeDtypeStruct((channels, cells), BF16)
    firsts, seconds = [], []
    for b in range(slots):
        branch0, hidden0, mask = pl.pallas_call(
            functools.partial(first_kernel, g, slots, planes, b),
            out_shape=[wide, wide, jax.ShapeDtypeStruct((AUG, g.width), F32)],
            in_specs=[whole()] * (5 + planes),
            out_specs=[whole()] * 3,
            scratch_shapes=[pltpu.VMEM((planes, slots, 2, rows, LANES), BF16)] + work,
            compiler_params=params(10),
            cost_estimate=cost(1 << 30),
        )(table, own, pick, weight, bias, *received)
        firsts.append((branch0, *neighbours_in_depth(branch0), hidden0, mask))
    for b in range(slots):
        branch1, kept = pl.pallas_call(
            functools.partial(second_kernel, g),
            out_shape=[narrow, narrow],
            in_specs=[whole()] * 9,
            out_specs=[whole()] * 2,
            scratch_shapes=work,
            compiler_params=params(10),
            cost_estimate=cost(1 << 30),
        )(*firsts[b], keep, weight, bias, dweight)
        seconds.append((branch1, *neighbours_in_depth(branch1), kept))
    out = None
    for b in range(slots):
        more = [] if out is None else [out]
        out = pl.pallas_call(
            functools.partial(last_kernel, blocks - 1, b),
            out_shape=jax.ShapeDtypeStruct(activations.shape, BF16),
            grid=(1,),
            in_specs=[whole()] * 7 + [hbm()] * len(more),
            out_specs=pl.BlockSpec((1, 1, channels, cells), lambda i, b=b: (b, 0, 0, 0)),
            input_output_aliases={7: 0} if more else {},
            compiler_params=params(),
            cost_estimate=cost(1 << 26),
        )(*seconds[b], aug, bias, dweight, *more)
    return out


def solution(mesh):
    in_specs = (
        P("plane", "depth", None, None),
        P(),
        P(),
        P(),
        P(),
        P(),
        P("plane", None),
        P("plane", "depth", None),
    )
    out_specs = P("plane", "depth", None, None)
    return jax.shard_map(shards, mesh=mesh, in_specs=in_specs, out_specs=out_specs, check_vma=False)
```
